768 devices in a mesh: dp: 12 (over x, z_lo), seq: 8 (over y), mp: 8 (over z_hi, core).
Axes of the slice: x: 4, y: 8, z: 12 (z_hi: 4, z_lo: 3; z = z_hi * 3 + z_lo), core: 2. Of those that a mesh axis runs over, the one named last changes fastest.
Arguments:
- inputs: bfloat16 [75264, 1024], P(('dp', 'seq', 'mp')), may hold values from -6 to 6
- grad_out: bfloat16 [75264, 1024], P(('dp', 'seq', 'mp')), may hold values from -6 to 6
- pad_mask: int32 [75264], P(('dp', 'seq', 'mp')), may hold values from 0 to 1, as said below
- hidden_pre: bfloat16 [75264, 4096], P(('dp', 'seq'), 'mp'), may hold values from -6 to 6
- w_in: bfloat16 [1024, 4096], P(None, 'mp'), may hold values from -0.1875 to 0.1875
- w_out: bfloat16 [4096, 1024], P('mp'), may hold values from -0.09375 to 0.09375
- ln_gain: float32 [1024], replicated, may hold values from 0.25 to 1.75
- ln_shift: float32 [1024], replicated, may hold values from -3 to 3
Outputs:
- grad_inputs: bfloat16 [75264, 1024], P(('dp', 'seq', 'mp'))
- grad_w_in: float32 [1024, 4096], P('seq', 'mp')
- grad_w_out: float32 [4096, 1024], P('mp', 'seq')
The draws below stay inside these ranges and needn't reach their ends.
Inputs may be any that keep to these rules, and one draw needn't show every extreme that they name: `pad_mask`: each window is 196 consecutive tokens, 14 rows of 14 in row order; its image tokens are those in its first h rows and first w columns, h and w between 4 and 14; some windows are full and some are not in every draw.
All inputs are finite; a program needn't handle non-finite values.
Results may differ from the reference program's by a relative error of at most 0.02.
Values may be sent and summed in bfloat16 or wider, within the bound.
No kernel may reach another device: no remote copies, remote signals or barrier semaphores. Data moves between devices by JAX's collectives and lax.ppermute only.
A program may use at most 32 MiB of HBM per device.

```python
import jax
import jax.numpy as jnp
from jax import lax

D = 1024
FF = 4096
WT = 196
TOKENS = 75264
N_MP = 8


def draw_pad_mask(key, part):
    windows = TOKENS // WT
    is_full = jax.random.randint(jax.random.fold_in(key, 11), (windows,), 0, 2)
    height = jax.random.randint(jax.random.fold_in(key, 12), (windows,), 4, 15)
    breadth = jax.random.randint(jax.random.fold_in(key, 13), (windows,), 4, 15)
    height = jnp.where(is_full == 1, 14, height)
    breadth = jnp.where(is_full == 1, 14, breadth)
    position = jnp.arange(WT, dtype=jnp.int32)
    row_pos = position // 14
    col_pos = position % 14
    alive_grid = (row_pos[None, :] < height[:, None]) & (col_pos[None, :] < breadth[:, None])
    return alive_grid.astype(jnp.int32).reshape(TOKENS)


def block_scale(rng, dims, pieces, least, high):
    def one(axis_at, parts):
        steps = jax.random.uniform(jax.random.fold_in(jax.random.fold_in(rng, 6), axis_at), (parts,), jnp.float32, least / len(pieces), high / len(pieces))
        return jnp.repeat(jnp.exp(steps), dims[axis_at] // parts).reshape((-1,) + (1,) * (len(dims) - axis_at - 1))

    loudness = one(*pieces[0])
    for cut in pieces[1:]:
        loudness = loudness * one(*cut)
    return loudness


def bell_draw(stream_key, dims, width, limit, cuts=(), kind=jnp.bfloat16):
    drawn = width * jax.random.normal(stream_key, dims, jnp.float32)
    if cuts:
        drawn = drawn * block_scale(stream_key, dims, cuts, -0.22, 0.18)
    return jnp.clip(drawn, -limit, limit).astype(kind)


def setup_inputs(seed: int = 0) -> dict:
    key_list = jax.random.split(jax.random.key(seed), 9)
    inputs = bell_draw(key_list[0], (TOKENS, D), 1.0, 6.0, ((0, 768),))
    grad_out = bell_draw(key_list[1], (TOKENS, D), 1.0, 6.0, ((0, 768),))
    pad_mask = draw_pad_mask(jax.random.fold_in(key_list[8], 71), 0)
    hidden_pre = bell_draw(key_list[3], (TOKENS, FF), 1.0, 6.0, ((0, 96), (1, 8)))
    w_in = bell_draw(key_list[4], (D, FF), D ** -0.5, 0.1875, ((1, 8),))
    w_out = bell_draw(key_list[5], (FF, D), FF ** -0.5, 0.09375, ((0, 8),))
    ln_gain = jnp.clip(1.0 + 0.15 * jax.random.normal(key_list[6], (D,), jnp.float32), 0.25, 1.75)
    ln_shift = bell_draw(key_list[7], (D,), 0.5, 3.0, (), jnp.float32)
    return {"inputs": inputs, "grad_out": grad_out, "pad_mask": pad_mask, "hidden_pre": hidden_pre, "w_in": w_in, "w_out": w_out, "ln_gain": ln_gain, "ln_shift": ln_shift}


EPSILON = 1e-06
ROOT_HALF = 0.7071067811865476
INV_ROOT_TAU = 0.3989422804014327

def gelu_pair(hidden_pre):
    values = hidden_pre.astype(jnp.float32)
    normal_cdf = 0.5 * (1.0 + lax.erf(values * ROOT_HALF))
    normal_pdf = jnp.exp(-0.5 * values * values) * INV_ROOT_TAU
    return (values * normal_cdf, normal_cdf + values * normal_pdf)

def layer_norm(inputs, ln_gain, ln_shift):
    values = inputs.astype(jnp.float32)
    row_mean = lax.optimization_barrier(jnp.mean(values, axis=1, keepdims=True))
    centred = values - row_mean
    row_var = lax.optimization_barrier(jnp.mean(centred * centred, axis=1, keepdims=True))
    inv_std = lax.rsqrt(row_var + EPSILON)
    x_hat = centred * inv_std
    normed = (x_hat * ln_gain + ln_shift).astype(jnp.bfloat16)
    return (x_hat, inv_std, normed)

def norm_backward(d_normed, x_hat, inv_std, ln_gain):
    d_hat = d_normed * ln_gain
    first_term = lax.optimization_barrier(jnp.mean(d_hat, axis=1, keepdims=True))
    second_term = lax.optimization_barrier(jnp.mean(d_hat * x_hat, axis=1, keepdims=True))
    return inv_std * (d_hat - first_term - x_hat * second_term)

def reference(inputs, grad_out, pad_mask, hidden_pre, w_in, w_out, ln_gain, ln_shift):
    x_hat, inv_std, normed = layer_norm(inputs, ln_gain, ln_shift)
    masked = (grad_out.astype(jnp.float32) * pad_mask.astype(jnp.float32)[:, None]).astype(jnp.bfloat16)
    activation, slope = gelu_pair(hidden_pre)
    activation = activation.astype(jnp.bfloat16)
    d_act = jnp.dot(masked, w_out.T, preferred_element_type=jnp.float32)
    d_hidden = (d_act * slope).astype(jnp.bfloat16)
    scale = float(TOKENS) ** (-0.5)
    grad_w_out = jnp.dot(activation.T, masked, preferred_element_type=jnp.float32) * scale
    grad_w_in = jnp.dot(normed.T, d_hidden, preferred_element_type=jnp.float32) * scale
    width_block = FF // N_MP
    d_normed = jnp.zeros((inputs.shape[0], D), jnp.float32)
    for shard in range(N_MP):
        left = d_hidden[:, shard * width_block:(shard + 1) * width_block]
        right = w_in[:, shard * width_block:(shard + 1) * width_block]
        partial_sum = jnp.dot(left, right.T, preferred_element_type=jnp.float32)
        partial_sum = lax.optimization_barrier(partial_sum.astype(jnp.bfloat16)).astype(jnp.float32)
        d_normed = d_normed + partial_sum
    grad_inputs = (masked.astype(jnp.float32) + norm_backward(d_normed, x_hat, inv_std, ln_gain)).astype(jnp.bfloat16)
    return (grad_inputs, grad_w_in, grad_w_out)
```

```python
import jax
import jax.numpy as jnp
from jax import lax
from jax.experimental import pallas as pl
from jax.experimental.pallas import tpu as pltpu
from jax.sharding import Mesh, PartitionSpec as P


EPSILON = 1e-06
ROOT_HALF = 0.7071067811865476
INV_ROOT_TAU = 0.3989422804014327


BF = jnp.bfloat16
LIMIT = 40 * 1024 * 1024
F32 = jnp.float32


def shifted(value, axis, step):
    n = lax.axis_size(axis)
    return lax.ppermute(value, axis, [(i, (i + step) % n) for i in range(n)])


def gelu_pair(hidden_pre):
    values = hidden_pre.astype(F32)
    normal_cdf = 0.5 * (1.0 + lax.erf(values * ROOT_HALF))
    normal_pdf = jnp.exp(-0.5 * values * values) * INV_ROOT_TAU
    return (values * normal_cdf, normal_cdf + values * normal_pdf)


NT = (((1,), (1,)), ((), ()))
NN = (((1,), (0,)), ((), ()))


def dot(a, b, dims):
    return lax.dot_general(a, b, dims, preferred_element_type=F32)


def in_hbm(body, outs, scratch, fetched, smem=()):
    ni, no, ns = len(fetched), len(outs), len(smem)

    def whole(*refs):
        scalars, src, dst = refs[:ns], refs[ns : ns + ni], refs[ns + ni : ns + ni + no]
        in_sem, out_sem, *rest = refs[ns + ni + no :]
        held, made, extra = rest[:ni], rest[ni : ni + no], rest[ni + no :]
        gets = [pltpu.make_async_copy(src[k], held[k], in_sem.at[k]) for k in range(ni)]
        puts = [pltpu.make_async_copy(made[k], dst[k], out_sem.at[k]) for k in range(no)]
        for g in gets:
            g.start()
        body(scalars, gets, puts, held, made, *extra)
        for p in puts:
            p.wait()

    hbm = pl.BlockSpec(memory_space=pltpu.HBM)
    return pl.pallas_call(
        whole,
        out_shape=[pltpu.HBM(v.shape, v.dtype) for v in outs],
        in_specs=[pl.BlockSpec(memory_space=pltpu.SMEM)] * ns + [hbm] * ni,
        out_specs=[hbm] * no,
        scratch_shapes=[
            pltpu.SemaphoreType.DMA((ni,)),
            pltpu.SemaphoreType.DMA((no,)),
            *[pltpu.VMEM(v.shape, v.dtype) for v in (*fetched, *outs)],
            *scratch,
        ],
        compiler_params=pltpu.CompilerParams(vmem_limit_bytes=LIMIT),
    )(*smem, *(pltpu.with_memory_space_constraint(v, pltpu.HBM) for v in fetched))


def shaped(shape, dtype=BF):
    return jax.ShapeDtypeStruct(shape, dtype)


def stack_rows(refs, spots, buf, rows, padded):
    d = buf.shape[1]
    for k, (which, lane) in enumerate(spots):
        at = k * padded
        buf[at + padded - 16 : at + padded, :] = jnp.zeros((16, d), buf.dtype)
        buf[at : at + rows, :] = refs[which][:, lane * d : (lane + 1) * d]


def norm_and_mask(inputs, grad_out, pad_mask, ln_gain, ln_shift):
    rows, d = inputs.shape

    def body(x_ref, g_ref, m_ref, gain_ref, shift_ref, out_ref):
        values = x_ref[...].astype(F32)
        centred = values - jnp.mean(values, axis=1, keepdims=True)
        row_var = jnp.mean(centred * centred, axis=1, keepdims=True)
        x_hat = centred * lax.rsqrt(row_var + EPSILON)
        out_ref[:, :d] = (g_ref[...].astype(F32) * m_ref[...].astype(F32)).astype(BF)
        out_ref[:, d:] = (x_hat * gain_ref[...] + shift_ref[...]).astype(BF)

    vmem = pl.BlockSpec(memory_space=pltpu.VMEM)
    return pl.pallas_call(
        body,
        out_shape=shaped((rows, 2 * d)),
        in_specs=[vmem] * 5,
        out_specs=vmem,
    )(inputs, grad_out, pad_mask[:, None], ln_gain[None], ln_shift[None])


def weight_terms(arrays, m_spots, n_spots, act_t, w_out, slope, x_idx, nx, ny, rows, padded):
    na, n = len(arrays), len(m_spots)
    ff, d = w_out.shape
    total, p, q = n * padded, ff // nx, d // ny

    def body(scalars, gets, puts, held, made, m_buf, n_buf, slabs):
        act_ref, wo_ref, slope_ref = held[na:]
        for g in gets[:na]:
            g.wait()
        stack_rows(held, m_spots, m_buf, rows, padded)
        stack_rows(held, n_spots, n_buf, rows, padded)
        m = m_buf[...]
        for g in gets[na:]:
            g.wait()
        dh = (dot(m, wo_ref[...], NT) * slope_ref[...]).astype(BF)
        made[nx][...] = dh
        puts[nx].start()
        t_out = dot(act_ref[...], m, NN).astype(BF)
        t_in = dot(dh.T, n_buf[...], NN).astype(BF)
        for k in range(nx):
            for j in range(ny):
                rk, cj = slice(k * p, (k + 1) * p), slice(j * q, (j + 1) * q)
                slabs[k, j, :q, :] = t_in[rk, cj].T
                slabs[k, j, q:, :] = t_out[rk, cj]
        for k in range(nx):
            made[k][...] = slabs[(scalars[0][0] + k) % nx]
            puts[k].start()

    assert p == q
    return in_hbm(
        body,
        [shaped((ny, 2 * q, p))] * nx + [shaped((total, ff))],
        [pltpu.VMEM((total, d), BF), pltpu.VMEM((total, d), BF), pltpu.VMEM((nx, ny, 2 * q, p), BF)],
        (*arrays, act_t, w_out, slope),
        (x_idx,),
    )


def input_grad(d_hidden, w_in, rows, padded):
    total, _ = d_hidden.shape
    d = w_in.shape[0]
    nh = total // padded // 2

    def body(_, gets, puts, held, made):
        for g in gets:
            g.wait()
        r = dot(held[0][...], held[1][...], NT).astype(BF)
        for half in (1, 0):
            for k in range(nh):
                at = (2 * k + half) * padded
                made[half][:, k * d : (k + 1) * d] = r[at : at + rows]
            puts[half].start()

    return in_hbm(body, [shaped((rows, nh * d))] * 2, [], (d_hidden, w_in))


def shards(inputs, grad_out, pad_mask, hidden_pre, w_in, w_out, ln_gain, ln_shift):
    rows, d = inputs.shape
    nh, nc = lax.axis_size("zh"), lax.axis_size("c")
    nx, ny, nz = lax.axis_size("x"), lax.axis_size("y"), lax.axis_size("zl")
    n = nh * nc
    ff = hidden_pre.shape[1]
    padded = -(-rows // 16) * 16
    both_own = norm_and_mask(inputs, grad_out, pad_mask, ln_gain, ln_shift)
    both3 = shifted(both_own, "zh", 1)
    both1 = shifted(both_own, "zh", -1)

    zh, c = lax.axis_index("zh"), lax.axis_index("c")
    h = hidden_pre.reshape(nh, nc, rows, ff)
    h = lax.dynamic_slice_in_dim(jnp.concatenate([h, h[:-1]], axis=0), zh, nh, axis=0)
    h = lax.dynamic_slice_in_dim(jnp.concatenate([h, h[:, :-1]], axis=1), c, nc, axis=1)
    h = jnp.pad(h.reshape(n, rows, ff), ((0, 0), (0, padded - rows), (0, 0)))
    activation, slope = gelu_pair(h.reshape(n * padded, ff))
    act_t = activation.astype(BF).T

    m2 = shifted(both3[:, :d], "zh", 1)
    n2 = shifted(both1[:, d:], "zh", -1)
    swaps = []
    for v in (both_own, both3, both1, jnp.concatenate([m2, n2], axis=1)):
        swaps.append(shifted(v, "c", 1))
    arrays = (both_own, swaps[0], both1, swaps[2], both3, swaps[1], swaps[3], m2, n2)

    def spots(k):
        return ((0, k), (1, k), (2, k), (3, k), (7 + k, 0), (6, k), (4, k), (5, k))

    x = lax.axis_index("x").astype(jnp.int32)
    *terms, d_hidden = weight_terms(
        arrays, spots(0), spots(1), act_t, w_out, slope, x.reshape(1), nx, ny, rows, padded
    )
    moved = {}
    for k in (1, 3, 2):
        moved[k] = shifted(terms[k], "x", k)
    dn_own, dn_other = input_grad(d_hidden, w_in, rows, padded)
    from_core = shifted(dn_other, "c", 1)

    def pair(k):
        lanes = slice(k * d, (k + 1) * d)
        return dn_own[:, lanes].astype(F32) + from_core[:, lanes].astype(F32)

    passing = shifted(pair(2).astype(BF), "zh", 1)
    from_up = shifted(pair(3).astype(BF), "zh", -1)
    from_down = shifted((pair(1) + passing.astype(F32)).astype(BF), "zh", 1)
    d_normed = pair(0) + from_up.astype(F32) + from_down.astype(F32)

    p, q = ff // nx, d // ny
    total = terms[0].astype(F32)
    for k in (1, 3, 2):
        total = total + moved[k].astype(F32)
    both_y = lax.all_to_all(total.astype(BF), "y", 0, 0, tiled=True)
    both = jnp.sum(both_y.astype(F32), axis=0).astype(BF)
    got = lax.all_to_all(
        jnp.broadcast_to(both, (nx * nz, *both.shape)), ("x", "zl"), 0, 0, tiled=True
    )
    whole = jnp.sum(got.reshape(nx, nz, 2, p, q).astype(F32), axis=1)

    values = inputs.astype(F32)
    row_mean = jnp.mean(values, axis=1, keepdims=True)
    centred = values - row_mean
    row_var = jnp.mean(centred * centred, axis=1, keepdims=True)
    inv_std = lax.rsqrt(row_var + EPSILON)
    x_hat = centred * inv_std
    d_hat = d_normed * ln_gain
    first_term = jnp.mean(d_hat, axis=1, keepdims=True)
    second_term = jnp.mean(d_hat * x_hat, axis=1, keepdims=True)
    grad_inputs = (
        both_own[:, :d].astype(F32) + inv_std * (d_hat - first_term - x_hat * second_term)
    ).astype(BF)

    scale = float(rows * n * nx * ny * nz) ** (-0.5)
    grad_w_out = whole[:, 1].reshape(ff, q) * scale
    grad_w_in = jnp.transpose(whole[:, 0], (1, 0, 2)).reshape(q, ff) * scale
    return (grad_inputs, grad_w_in, grad_w_out)


RUN = 3


def solution(mesh):
    dp, seq, mp = (mesh.shape[a] for a in ("dp", "seq", "mp"))
    fine = Mesh(mesh.devices.reshape(dp // RUN, RUN, seq, mp // 2, 2), ("x", "zl", "y", "zh", "c"))
    tokens = ("x", "zl", "y")
    hidden = ("zh", "c")

    return jax.shard_map(
        shards,
        mesh=fine,
        in_specs=(
            P((*tokens, *hidden), None),
            P((*tokens, *hidden), None),
            P((*tokens, *hidden)),
            P(tokens, hidden),
            P(None, hidden),
            P(hidden, None),
            P(),
            P(),
        ),
        out_specs=(P((*tokens, *hidden), None), P("y", hidden), P(hidden, "y")),
        check_vma=False,
    )
```

```python
import jax
import jax.numpy as jnp
from jax import lax
from jax.experimental import pallas as pl
from jax.experimental.pallas import tpu as pltpu
from jax.sharding import Mesh, PartitionSpec as P


EPSILON = 1e-06
ROOT_HALF = 0.7071067811865476
INV_ROOT_TAU = 0.3989422804014327


BF = jnp.bfloat16
LIMIT = 40 * 1024 * 1024
F32 = jnp.float32


def shifted(value, axis, step):
    n = lax.axis_size(axis)
    return lax.ppermute(value, axis, [(i, (i + step) % n) for i in range(n)])


def gelu_pair(hidden_pre):
    values = hidden_pre.astype(F32)
    normal_cdf = 0.5 * (1.0 + lax.erf(values * ROOT_HALF))
    normal_pdf = jnp.exp(-0.5 * values * values) * INV_ROOT_TAU
    return (values * normal_cdf, normal_cdf + values * normal_pdf)


NT = (((1,), (1,)), ((), ()))
NN = (((1,), (0,)), ((), ()))


def dot(a, b, dims):
    return lax.dot_general(a, b, dims, preferred_element_type=F32)


def in_hbm(body, outs, scratch, fetched, smem=(), loose=()):
    ni, no, ns = len(fetched), len(outs), len(smem)

    def whole(*refs):
        scalars, src, dst = refs[:ns], refs[ns : ns + ni], refs[ns + ni : ns + ni + no]
        in_sem, out_sem, *rest = refs[ns + ni + no :]
        held, made, extra = rest[:ni], rest[ni : ni + no], rest[ni + no :]
        gets = [pltpu.make_async_copy(src[k], held[k], in_sem.at[k]) for k in range(ni)]
        puts = [pltpu.make_async_copy(made[k], dst[k], out_sem.at[k]) for k in range(no)]
        for g in gets:
            g.start()
        body(scalars, gets, puts, held, made, *extra)
        for p in puts:
            p.wait()

    hbm = pl.BlockSpec(memory_space=pltpu.HBM)
    return pl.pallas_call(
        whole,
        out_shape=[pltpu.HBM(v.shape, v.dtype) for v in outs],
        in_specs=[pl.BlockSpec(memory_space=pltpu.SMEM)] * ns
        + [pl.BlockSpec(memory_space=pl.ANY) if k in loose else hbm for k in range(ni)],
        out_specs=[hbm] * no,
        scratch_shapes=[
            pltpu.SemaphoreType.DMA((ni,)),
            pltpu.SemaphoreType.DMA((no,)),
            *[pltpu.VMEM(v.shape, v.dtype) for v in (*fetched, *outs)],
            *scratch,
        ],
        compiler_params=pltpu.CompilerParams(vmem_limit_bytes=LIMIT),
    )(
        *smem,
        *(
            v if k in loose else pltpu.with_memory_space_constraint(v, pltpu.HBM)
            for k, v in enumerate(fetched)
        ),
    )


def shaped(shape, dtype=BF):
    return jax.ShapeDtypeStruct(shape, dtype)


def stack_rows(refs, spots, buf, rows, padded):
    d = buf.shape[1]
    for k, (which, lane) in enumerate(spots):
        at = k * padded
        buf[at + padded - 16 : at + padded, :] = jnp.zeros((16, d), buf.dtype)
        buf[at : at + rows, :] = refs[which][:, lane * d : (lane + 1) * d]


def norm_and_mask(inputs, grad_out, pad_mask, ln_gain, ln_shift):
    rows, d = inputs.shape

    def body(x_ref, g_ref, m_ref, gain_ref, shift_ref, out_ref):
        values = x_ref[...].astype(F32)
        centred = values - jnp.mean(values, axis=1, keepdims=True)
        row_var = jnp.mean(centred * centred, axis=1, keepdims=True)
        x_hat = centred * lax.rsqrt(row_var + EPSILON)
        square = [lax.broadcasted_iota(jnp.int32, (rows, rows), k) for k in (0, 1)]
        diagonal = jnp.where(square[0] == square[1], m_ref[...].astype(F32), 0.0)
        mask = jnp.sum(diagonal, axis=1, keepdims=True)
        out_ref[:, :d] = (g_ref[...].astype(F32) * mask).astype(BF)
        out_ref[:, d:] = (x_hat * gain_ref[...] + shift_ref[...]).astype(BF)

    vmem = pl.BlockSpec(memory_space=pltpu.VMEM)
    return pl.pallas_call(
        body,
        out_shape=shaped((rows, 2 * d)),
        in_specs=[vmem] * 5,
        out_specs=vmem,
    )(inputs, grad_out, pad_mask[None], ln_gain[None], ln_shift[None])


def weight_terms(arrays, m_spots, n_spots, act_t, w_out, slope, x_idx, nx, ny, rows, padded):
    na, n = len(arrays), len(m_spots)
    ff, d = w_out.shape
    total, p, q = n * padded, ff // nx, d // ny

    def body(scalars, gets, puts, held, made, m_buf, n_buf, slabs):
        act_ref, wo_ref, slope_ref = held[na:]
        for g in gets[:na]:
            g.wait()
        stack_rows(held, m_spots, m_buf, rows, padded)
        stack_rows(held, n_spots, n_buf, rows, padded)
        m = m_buf[...]
        for g in gets[na:]:
            g.wait()
        dh = (dot(m, wo_ref[...], NT) * slope_ref[...]).astype(BF)
        made[nx][...] = dh
        puts[nx].start()
        t_out = dot(act_ref[...], m, NN).astype(BF)
        t_in = dot(dh.T, n_buf[...], NN).astype(BF)
        for k in range(nx):
            for j in range(ny):
                rk, cj = slice(k * p, (k + 1) * p), slice(j * q, (j + 1) * q)
                slabs[k, j, :q, :] = t_in[rk, cj].T
                slabs[k, j, q:, :] = t_out[rk, cj]
        for k in range(nx):
            made[k][...] = slabs[(scalars[0][0] + k) % nx]
            puts[k].start()

    assert p == q
    return in_hbm(
        body,
        [shaped((ny, 2 * q, p))] * nx + [shaped((total, ff))],
        [pltpu.VMEM((total, d), BF), pltpu.VMEM((total, d), BF), pltpu.VMEM((nx, ny, 2 * q, p), BF)],
        (*arrays, act_t, w_out, slope),
        (x_idx,),
        (6,),
    )


def input_grad(d_hidden, w_in, rows, padded):
    total, _ = d_hidden.shape
    d = w_in.shape[0]
    nh = total // padded // 2

    def body(_, gets, puts, held, made):
        for g in gets:
            g.wait()
        r = dot(held[0][...], held[1][...], NT).astype(BF)
        for half in (1, 0):
            for k in range(nh):
                at = (2 * k + half) * padded
                made[half][:, k * d : (k + 1) * d] = r[at : at + rows]
            puts[half].start()

    return in_hbm(body, [shaped((rows, nh * d))] * 2, [], (d_hidden, w_in))


def shards(inputs, grad_out, pad_mask, hidden_pre, w_in, w_out, ln_gain, ln_shift):
    rows, d = inputs.shape
    nh, nc = lax.axis_size("zh"), lax.axis_size("c")
    nx, ny, nz = lax.axis_size("x"), lax.axis_size("y"), lax.axis_size("zl")
    n = nh * nc
    ff = hidden_pre.shape[1]
    padded = -(-rows // 16) * 16
    both_own = norm_and_mask(inputs, grad_out, pad_mask, ln_gain, ln_shift)
    both3 = shifted(both_own, "zh", 1)
    both1 = shifted(both_own, "zh", -1)

    zh, c = lax.axis_index("zh"), lax.axis_index("c")
    h = hidden_pre.reshape(nh, nc, rows, ff)
    h = lax.dynamic_slice_in_dim(jnp.concatenate([h, h[:-1]], axis=0), zh, nh, axis=0)
    h = lax.dynamic_slice_in_dim(jnp.concatenate([h, h[:, :-1]], axis=1), c, nc, axis=1)
    h = jnp.pad(h.reshape(n, rows, ff), ((0, 0), (0, padded - rows), (0, 0)))
    activation, slope = gelu_pair(h.reshape(n * padded, ff))
    act_t = activation.astype(BF).T

    m2 = shifted(both3[:, :d], "zh", 1)
    n2 = shifted(both1[:, d:], "zh", -1)
    swaps = []
    for v in (both_own, both3, both1, jnp.concatenate([m2, n2], axis=1)):
        swaps.append(shifted(v, "c", 1))
    arrays = (both_own, swaps[0], both1, swaps[2], both3, swaps[1], swaps[3], m2, n2)

    def spots(k):
        return ((0, k), (1, k), (2, k), (3, k), (7 + k, 0), (6, k), (4, k), (5, k))

    x = lax.axis_index("x").astype(jnp.int32)
    *terms, d_hidden = weight_terms(
        arrays, spots(0), spots(1), act_t, w_out, slope, x.reshape(1), nx, ny, rows, padded
    )
    moved = {}
    for k in (1, 3, 2):
        moved[k] = shifted(terms[k], "x", k)
    dn_own, dn_other = input_grad(d_hidden, w_in, rows, padded)
    from_core = shifted(dn_other, "c", 1)

    def pair(k):
        lanes = slice(k * d, (k + 1) * d)
        return dn_own[:, lanes].astype(F32) + from_core[:, lanes].astype(F32)

    passing = shifted(pair(2).astype(BF), "zh", 1)
    from_up = shifted(pair(3).astype(BF), "zh", -1)
    from_down = shifted((pair(1) + passing.astype(F32)).astype(BF), "zh", 1)
    d_normed = pair(0) + from_up.astype(F32) + from_down.astype(F32)

    total = terms[0].astype(F32)
    for k in (1, 3, 2):
        total = total + moved[k].astype(F32)
    both_y = lax.all_to_all(total.astype(BF), "y", 0, 0, tiled=True)
    both = jnp.sum(both_y.astype(F32), axis=0).astype(BF)
    got = lax.all_to_all(
        jnp.broadcast_to(both, (nx * nz, *both.shape)), ("x", "zl"), 0, 0, tiled=True
    )
    p, q = ff // nx, d // ny
    scale = float(rows * n * nx * ny * nz) ** (-0.5)
    whole = jnp.sum(got.reshape(nx, nz, 2, q, p).astype(F32), axis=1)
    grad_w_in = jnp.transpose(whole[:, 0], (1, 0, 2)).reshape(q, ff) * scale
    grad_w_out = whole[:, 1].reshape(ff, q) * scale

    values = inputs.astype(F32)
    row_mean = jnp.mean(values, axis=1, keepdims=True)
    centred = values - row_mean
    row_var = jnp.mean(centred * centred, axis=1, keepdims=True)
    inv_std = lax.rsqrt(row_var + EPSILON)
    x_hat = centred * inv_std
    d_hat = d_normed * ln_gain
    first_term = jnp.mean(d_hat, axis=1, keepdims=True)
    second_term = jnp.mean(d_hat * x_hat, axis=1, keepdims=True)
    grad_inputs = (
        both_own[:, :d].astype(F32) + inv_std * (d_hat - first_term - x_hat * second_term)
    ).astype(BF)

    return (grad_inputs, grad_w_in, grad_w_out)


RUN = 3


def solution(mesh):
    dp, seq, mp = (mesh.shape[a] for a in ("dp", "seq", "mp"))
    fine = Mesh(mesh.devices.reshape(dp // RUN, RUN, seq, mp // 2, 2), ("x", "zl", "y", "zh", "c"))
    tokens = ("x", "zl", "y")
    hidden = ("zh", "c")

    return jax.shard_map(
        shards,
        mesh=fine,
        in_specs=(
            P((*tokens, *hidden), None),
            P((*tokens, *hidden), None),
            P((*tokens, *hidden)),
            P(tokens, hidden),
            P(None, hidden),
            P(hidden, None),
            P(),
            P(),
        ),
        out_specs=(P((*tokens, *hidden), None), P("y", hidden), P(hidden, "y")),
        check_vma=False,
    )
```

```python
import jax
import jax.numpy as jnp
from jax import lax
from jax.experimental import pallas as pl
from jax.experimental.pallas import tpu as pltpu
from jax.sharding import Mesh, PartitionSpec as P


EPSILON = 1e-06
ROOT_HALF = 0.7071067811865476
INV_ROOT_TAU = 0.3989422804014327


BF = jnp.bfloat16
LIMIT = 40 * 1024 * 1024
F32 = jnp.float32


def shifted(value, axis, step):
    n = lax.axis_size(axis)
    return lax.ppermute(value, axis, [(i, (i + step) % n) for i in range(n)])


def mirrored(value, step):
    n, nc = lax.axis_size("zh"), lax.axis_size("c")
    pairs = [
        (i * nc + c, (i + (step if c == 0 else -step)) % n * nc + c)
        for i in range(n)
        for c in range(nc)
    ]
    return lax.ppermute(value, ("zh", "c"), pairs)


def gelu_pair(hidden_pre):
    values = hidden_pre.astype(F32)
    normal_cdf = 0.5 * (1.0 + lax.erf(values * ROOT_HALF))
    normal_pdf = jnp.exp(-0.5 * values * values) * INV_ROOT_TAU
    return (values * normal_cdf, normal_cdf + values * normal_pdf)


NT = (((1,), (1,)), ((), ()))
NN = (((1,), (0,)), ((), ()))


def dot(a, b, dims):
    return lax.dot_general(a, b, dims, preferred_element_type=F32)


def in_hbm(body, outs, scratch, fetched, smem=(), loose=()):
    ni, no, ns = len(fetched), len(outs), len(smem)

    def whole(*refs):
        scalars, src, dst = refs[:ns], refs[ns : ns + ni], refs[ns + ni : ns + ni + no]
        in_sem, out_sem, *rest = refs[ns + ni + no :]
        held, made, extra = rest[:ni], rest[ni : ni + no], rest[ni + no :]
        gets = [pltpu.make_async_copy(src[k], held[k], in_sem.at[k]) for k in range(ni)]
        puts = [pltpu.make_async_copy(made[k], dst[k], out_sem.at[k]) for k in range(no)]
        for g in gets:
            g.start()
        body(scalars, gets, puts, held, made, *extra)
        for p in puts:
            p.wait()

    hbm = pl.BlockSpec(memory_space=pltpu.HBM)
    return pl.pallas_call(
        whole,
        out_shape=[pltpu.HBM(v.shape, v.dtype) for v in outs],
        in_specs=[pl.BlockSpec(memory_space=pltpu.SMEM)] * ns
        + [pl.BlockSpec(memory_space=pl.ANY) if k in loose else hbm for k in range(ni)],
        out_specs=[hbm] * no,
        scratch_shapes=[
            pltpu.SemaphoreType.DMA((ni,)),
            pltpu.SemaphoreType.DMA((no,)),
            *[pltpu.VMEM(v.shape, v.dtype) for v in (*fetched, *outs)],
            *scratch,
        ],
        compiler_params=pltpu.CompilerParams(vmem_limit_bytes=LIMIT),
    )(
        *smem,
        *(
            v if k in loose else pltpu.with_memory_space_constraint(v, pltpu.HBM)
            for k, v in enumerate(fetched)
        ),
    )


def shaped(shape, dtype=BF):
    return jax.ShapeDtypeStruct(shape, dtype)


def stack_rows(refs, spots, buf, rows, padded):
    d = buf.shape[1]
    for k, (which, lane) in enumerate(spots):
        at = k * padded
        buf[at + padded - 16 : at + padded, :] = jnp.zeros((16, d), buf.dtype)
        buf[at : at + rows, :] = refs[which][:, lane * d : (lane + 1) * d]


def norm_and_mask(inputs, grad_out, pad_mask, ln_gain, ln_shift):
    rows, d = inputs.shape

    def body(x_ref, g_ref, m_ref, gain_ref, shift_ref, out_ref):
        values = x_ref[...].astype(F32)
        centred = values - jnp.mean(values, axis=1, keepdims=True)
        row_var = jnp.mean(centred * centred, axis=1, keepdims=True)
        x_hat = centred * lax.rsqrt(row_var + EPSILON)
        square = [lax.broadcasted_iota(jnp.int32, (rows, rows), k) for k in (0, 1)]
        diagonal = jnp.where(square[0] == square[1], m_ref[...].astype(F32), 0.0)
        mask = jnp.sum(diagonal, axis=1, keepdims=True)
        out_ref[:, :d] = (g_ref[...].astype(F32) * mask).astype(BF)
        out_ref[:, d:] = (x_hat * gain_ref[...] + shift_ref[...]).astype(BF)

    vmem = pl.BlockSpec(memory_space=pltpu.VMEM)
    return pl.pallas_call(
        body,
        out_shape=shaped((rows, 2 * d)),
        in_specs=[vmem] * 5,
        out_specs=vmem,
    )(inputs, grad_out, pad_mask[None], ln_gain[None], ln_shift[None])


def weight_terms(arrays, m_spots, n_spots, act_t, w_out, slope, x_idx, nx, ny, rows, padded):
    na, n = len(arrays), len(m_spots)
    ff, d = w_out.shape
    total, p, q = n * padded, ff // nx, d // ny

    def body(scalars, gets, puts, held, made, m_buf, n_buf, slabs):
        act_ref, wo_ref, slope_ref = held[na:]
        for g in gets[:na]:
            g.wait()
        stack_rows(held, m_spots, m_buf, rows, padded)
        stack_rows(held, n_spots, n_buf, rows, padded)
        m = m_buf[...]
        for g in gets[na:]:
            g.wait()
        dh = (dot(m, wo_ref[...], NT) * slope_ref[...]).astype(BF)
        made[nx][...] = dh
        puts[nx].start()
        t_out = dot(act_ref[...], m, NN).astype(BF)
        t_in = dot(dh.T, n_buf[...], NN).astype(BF)
        for k in range(nx):
            for j in range(ny):
                rk, cj = slice(k * p, (k + 1) * p), slice(j * q, (j + 1) * q)
                slabs[k, j, :q, :] = t_in[rk, cj].T
                slabs[k, j, q:, :] = t_out[rk, cj]
        for k in range(nx):
            made[k][...] = slabs[(scalars[0][0] + k) % nx]
            puts[k].start()

    assert p == q
    return in_hbm(
        body,
        [shaped((ny, 2 * q, p))] * nx + [shaped((total, ff))],
        [pltpu.VMEM((total, d), BF), pltpu.VMEM((total, d), BF), pltpu.VMEM((nx, ny, 2 * q, p), BF)],
        (*arrays, act_t, w_out, slope),
        (x_idx,),
        (6,),
    )


def input_grad(d_hidden, w_in, rows, padded):
    total, _ = d_hidden.shape
    d = w_in.shape[0]
    nh = total // padded // 2

    def body(_, gets, puts, held, made):
        for g in gets:
            g.wait()
        r = dot(held[0][...], held[1][...], NT).astype(BF)
        for half in (1, 0):
            for k in range(nh):
                at = (2 * k + half) * padded
                made[half][:, k * d : (k + 1) * d] = r[at : at + rows]
            puts[half].start()

    return in_hbm(body, [shaped((rows, nh * d))] * 2, [], (d_hidden, w_in))


def shards(inputs, grad_out, pad_mask, hidden_pre, w_in, w_out, ln_gain, ln_shift):
    rows, d = inputs.shape
    nh, nc = lax.axis_size("zh"), lax.axis_size("c")
    nx, ny, nz = lax.axis_size("x"), lax.axis_size("y"), lax.axis_size("zl")
    n = nh * nc
    ff = hidden_pre.shape[1]
    padded = -(-rows // 16) * 16
    both_own = norm_and_mask(inputs, grad_out, pad_mask, ln_gain, ln_shift)
    both3 = mirrored(both_own, 1)
    both1 = mirrored(both_own, -1)

    zh, c = lax.axis_index("zh"), lax.axis_index("c")
    h = hidden_pre.reshape(nh, nc, rows, ff)
    first = jnp.where(c == 0, zh, nh - 1 - zh)
    h = jnp.where(c == 0, h, h[::-1])
    h = lax.dynamic_slice_in_dim(jnp.concatenate([h, h[:-1]], axis=0), first, nh, axis=0)
    h = lax.dynamic_slice_in_dim(jnp.concatenate([h, h[:, :-1]], axis=1), c, nc, axis=1)
    h = jnp.pad(h.reshape(n, rows, ff), ((0, 0), (0, padded - rows), (0, 0)))
    activation, slope = gelu_pair(h.reshape(n * padded, ff))
    act_t = activation.astype(BF).T

    m2 = mirrored(both3[:, :d], 1)
    n2 = mirrored(both1[:, d:], -1)
    swaps = []
    for v in (both_own, both3, both1, jnp.concatenate([m2, n2], axis=1)):
        swaps.append(shifted(v, "c", 1))
    arrays = (both_own, swaps[0], both1, swaps[1], both3, swaps[2], swaps[3], m2, n2)

    def spots(k):
        return ((0, k), (1, k), (2, k), (3, k), (7 + k, 0), (6, k), (4, k), (5, k))

    x = lax.axis_index("x").astype(jnp.int32)
    *terms, d_hidden = weight_terms(
        arrays, spots(0), spots(1), act_t, w_out, slope, x.reshape(1), nx, ny, rows, padded
    )
    moved = {}
    for k in (1, 3, 2):
        moved[k] = shifted(terms[k], "x", k)
    dn_own, dn_other = input_grad(d_hidden, w_in, rows, padded)
    from_core = shifted(dn_other, "c", 1)

    def pair(k):
        mine, theirs = (slice(j * d, (j + 1) * d) for j in (k, -k % nh))
        return dn_own[:, mine].astype(F32) + from_core[:, theirs].astype(F32)

    passing = mirrored(pair(2).astype(BF), 1)
    from_up = mirrored(pair(3).astype(BF), -1)
    from_down = mirrored((pair(1) + passing.astype(F32)).astype(BF), 1)
    d_normed = pair(0) + from_up.astype(F32) + from_down.astype(F32)

    total = terms[0].astype(F32)
    for k in (1, 3, 2):
        total = total + moved[k].astype(F32)
    both_y = lax.all_to_all(total.astype(BF), "y", 0, 0, tiled=True)
    both = jnp.sum(both_y.astype(F32), axis=0).astype(BF)
    got = lax.all_to_all(
        jnp.broadcast_to(both, (nx * nz, *both.shape)), ("x", "zl"), 0, 0, tiled=True
    )
    p, q = ff // nx, d // ny
    scale = float(rows * n * nx * ny * nz) ** (-0.5)
    whole = jnp.sum(got.reshape(nx, nz, 2, q, p).astype(F32), axis=1)
    grad_w_in = jnp.transpose(whole[:, 0], (1, 0, 2)).reshape(q, ff) * scale
    grad_w_out = whole[:, 1].reshape(ff, q) * scale

    values = inputs.astype(F32)
    row_mean = jnp.mean(values, axis=1, keepdims=True)
    centred = values - row_mean
    row_var = jnp.mean(centred * centred, axis=1, keepdims=True)
    inv_std = lax.rsqrt(row_var + EPSILON)
    x_hat = centred * inv_std
    d_hat = d_normed * ln_gain
    first_term = jnp.mean(d_hat, axis=1, keepdims=True)
    second_term = jnp.mean(d_hat * x_hat, axis=1, keepdims=True)
    grad_inputs = (
        both_own[:, :d].astype(F32) + inv_std * (d_hat - first_term - x_hat * second_term)
    ).astype(BF)

    return (grad_inputs, grad_w_in, grad_w_out)


RUN = 3


def solution(mesh):
    dp, seq, mp = (mesh.shape[a] for a in ("dp", "seq", "mp"))
    fine = Mesh(mesh.devices.reshape(dp // RUN, RUN, seq, mp // 2, 2), ("x", "zl", "y", "zh", "c"))
    tokens = ("x", "zl", "y")
    hidden = ("zh", "c")

    return jax.shard_map(
        shards,
        mesh=fine,
        in_specs=(
            P((*tokens, *hidden), None),
            P((*tokens, *hidden), None),
            P((*tokens, *hidden)),
            P(tokens, hidden),
            P(None, hidden),
            P(hidden, None),
            P(),
            P(),
        ),
        out_specs=(P((*tokens, *hidden), None), P("y", hidden), P(hidden, "y")),
        check_vma=False,
    )
```
